32 devices in a mesh: trial: 2 (over core), bank: 4 (over y, x), zero: 4 (over z).
Axes of the slice: x: 2, y: 2, z: 4, core: 2. Of those that a mesh axis runs over, the one named last changes fastest.
Arguments:
- w_gate: float32 [128, 2048, 1024], P(('trial', 'bank'), 'zero'), parts along dimension 0, may hold values from -0.1875 to 0.1875
- w_up: float32 [128, 2048, 1024], P(('trial', 'bank'), 'zero'), parts along dimension 0, may hold values from -0.1875 to 0.1875
- router_weight: float32 [4096, 64], P(('trial', 'zero'), 'bank'), parts along dimension 0, may hold values from -0.125 to 0.125
- router_gain: float32 [4096], P(('trial', 'zero')), parts along dimension 0, may hold values from 0.25 to 1.75
Outputs:
- serve_gate: bfloat16 [128, 2048, 1024], P(('trial', 'bank'), None, 'zero'), parts along dimension 0
- serve_up: bfloat16 [128, 2048, 1024], P(('trial', 'bank'), None, 'zero'), parts along dimension 0
- scale_gate: float32 [128, 1024], P(('trial', 'bank'), 'zero'), parts along dimension 0
- scale_up: float32 [128, 1024], P(('trial', 'bank'), 'zero'), parts along dimension 0
- serve_router: bfloat16 [4096, 64], P('trial'), parts along dimension 0
The draws below stay inside these ranges and needn't reach their ends.
There are 2 independent parts, one for each index of `trial`. The reference program is written for one: setup_inputs(seed, part) draws one part's arguments, and reference() takes and returns one part's arrays. A program takes and returns all parts, laid end to end along the dimension named above; each array names one. Nothing has to cross between parts.
All inputs are finite; a program needn't handle non-finite values. Where the reference program divides by a largest or mean magnitude, that divisor is 1e-20 or more.
Results may differ from the reference program's by a relative error of at most 0.001.
Values may be sent and summed in bfloat16 or wider, within the bound.
A program may use at most 192 MiB of HBM per device.

```python
import jax
import jax.numpy as jnp

EXPERTS = 64
D_MODEL = 2048
D_EXPERT = 1024


def spiked(drawn, key, source, target, parts, factor):
    def block_of(position):
        return (jnp.arange(drawn.shape[position]) // (drawn.shape[position] // parts)).reshape((-1,) + (1,) * (drawn.ndim - 1 - position))

    near = jax.random.permutation(key, parts)[block_of(target)]
    other_side = (block_of(target) + parts // 2) % parts
    return jnp.where((block_of(source) == near) | (block_of(source) == other_side), factor * drawn, drawn)


def level_of(stream_key, dims, cuts, least, top_value):
    def one(dim, parts):
        heights = jax.random.uniform(jax.random.fold_in(jax.random.fold_in(stream_key, 6), dim), (parts,), jnp.float32, least / len(cuts), top_value / len(cuts))
        return jnp.repeat(jnp.exp(heights), dims[dim] // parts).reshape((-1,) + (1,) * (len(dims) - dim - 1))

    gain = one(*cuts[0])
    for cut in cuts[1:]:
        gain = gain * one(*cut)
    return gain


def noise(stream_key, dims, spread, bound, shards=(), held_as=jnp.bfloat16):
    gain = level_of(stream_key, dims, shards, -0.22, 0.18) if shards else 1.0
    entries = jax.random.normal(stream_key, dims, jnp.float32) * spread * gain
    return jnp.minimum(jnp.maximum(entries, -bound), bound).astype(held_as)


def noise_with(rng, extent, width, most, cuts, heavy, kind=jnp.bfloat16):
    array = width * jax.random.normal(rng, extent, jnp.float32)
    if cuts:
        array = array * level_of(rng, extent, cuts, -0.22, 0.18)
    return jnp.clip(spiked(array, jax.random.fold_in(rng, 3), *heavy), -most, most).astype(kind)


def setup_inputs(seed: int = 0, part: int = 0) -> dict:
    arg_keys = jax.random.split(jax.random.key(seed), 5)
    part_splits = jax.random.split(jax.random.fold_in(arg_keys[4], part), 5)
    return {
        "w_gate": noise_with(part_splits[0], (EXPERTS, D_MODEL, D_EXPERT), D_MODEL ** -0.5, 0.1875, ((0, 4), (1, 4)), (1, 2, 4, 2.0), jnp.float32),
        "w_up": noise_with(part_splits[1], (EXPERTS, D_MODEL, D_EXPERT), D_MODEL ** -0.5, 0.1875, ((0, 4), (1, 4)), (1, 2, 4, 2.0), jnp.float32),
        "router_weight": noise(part_splits[2], (D_MODEL, EXPERTS), D_MODEL ** -0.5, 0.125, ((0, 4), (1, 4)), jnp.float32),
        "router_gain": jnp.clip(1.0 + 0.15 * jax.random.normal(part_splits[3], (D_MODEL,), jnp.float32), 0.25, 1.75),
    }


def reference(w_gate, w_up, router_weight, router_gain):
    scale_gate = jnp.sum(jnp.abs(w_gate), axis=1) / D_MODEL
    serve_gate = (w_gate / jnp.expand_dims(scale_gate, 1)).astype(jnp.bfloat16)
    scale_up = jnp.sum(jnp.abs(w_up), axis=1) / D_MODEL
    serve_up = (w_up / jnp.expand_dims(scale_up, 1)).astype(jnp.bfloat16)
    serve_router = (router_weight * router_gain[:, None]).astype(jnp.bfloat16)
    return serve_gate, serve_up, scale_gate, scale_up, serve_router
```

```python
import functools

import jax
import jax.numpy as jnp
from jax import lax
from jax.experimental import pallas as pl
from jax.experimental.pallas import tpu as pltpu
from jax.sharding import PartitionSpec as P

MESH = pl.DeviceIdType.MESH
SLOTS = 3
STEP = 16


def plain(n, w_gate, w_up, router_weight, router_gain):
    d_model = w_gate.shape[1] * n

    def rescaled(w):
        scale = lax.psum(jnp.sum(jnp.abs(w), axis=1), "zero") / d_model
        narrow = (w / jnp.expand_dims(scale, 1)).astype(jnp.bfloat16)
        serve = lax.all_to_all(narrow, "zero", split_axis=2, concat_axis=1, tiled=True)
        width = serve.shape[2]
        return serve, lax.dynamic_slice_in_dim(scale, lax.axis_index("zero") * width, width, axis=1)

    serve_gate, scale_gate = rescaled(w_gate)
    serve_up, scale_up = rescaled(w_up)
    part = (router_weight * router_gain[:, None]).astype(jnp.bfloat16)
    row = lax.all_gather(part, "zero", axis=0, tiled=True)
    router = lax.all_gather(row, "bank", axis=1, tiled=True)
    return serve_gate, serve_up, scale_gate, scale_up, router


def kernel(
    n, banks, wg_ref, wu_ref, rw_ref, rg_ref,
    og_ref, ou_ref, sg_ref, su_ref, rt_ref,
    stage, first, sendbuf, parts, scales,
    in_sem, first_sem, own_sem, send_sem, recv_sem, x_send, x_recv, rz_send, rz_recv, rb_send, rb_recv,
):
    me = lax.axis_index("zero")
    bank = lax.axis_index("bank")
    w, o, so = (wg_ref, wu_ref), (og_ref, ou_ref), (sg_ref, su_ref)
    experts, rows, cols = wg_ref.shape
    width = cols // n
    d_model = rows * n

    for m in range(2):
        pltpu.make_async_copy(w[m].at[0], first.at[m], first_sem.at[m]).start()

    def load(m, e, slot):
        return pltpu.make_async_copy(w[m].at[e], stage.at[m, slot], in_sem.at[m, slot])

    for e in range(1, min(1 + SLOTS, experts)):
        for m in range(2):
            load(m, e, e % SLOTS).start()

    def others(axis, here, count, act):
        for p in range(count):
            @pl.when(here != p)
            def _():
                act(p)

    barrier = pltpu.get_barrier_semaphore()

    def greet(axis):
        return lambda p: pl.semaphore_signal(barrier, inc=1, device_id={axis: p}, device_id_type=MESH)

    others("zero", me, n, greet("zero"))
    others("bank", bank, banks, greet("bank"))

    def stats(src, m, e):
        def body(r, acc):
            return acc + jnp.abs(src[pl.ds(pl.multiple_of(r * 8, 8), 8), :])

        acc = lax.fori_loop(0, rows // 8, body, jnp.zeros((8, cols), jnp.float32), unroll=8)
        parts[me, e, m] = jnp.sum(acc, axis=0, keepdims=True)

    def chunk(ref, s, g):
        if g < 2:
            return ref.at[s, 0, g]
        return ref.at[s, pl.ds(1, experts - 1)]

    def swap(g, p):
        return pltpu.make_async_remote_copy(
            src_ref=chunk(parts, me, g), dst_ref=chunk(parts, me, g),
            send_sem=x_send.at[g, p], recv_sem=x_recv.at[g, me],
            device_id={"zero": p}, device_id_type=MESH,
        )

    def swapped(g, p):
        return pltpu.make_async_remote_copy(
            src_ref=chunk(parts, p, g), dst_ref=chunk(parts, p, g),
            send_sem=x_send.at[g, p], recv_sem=x_recv.at[g, p],
            device_id={"zero": p}, device_id_type=MESH,
        )

    def narrow(src, m, e):
        total = parts[0, e, m]
        for s in range(1, n):
            total = total + parts[s, e, m]
        scale = total / d_model
        scales[...] = scale
        so[m][pl.ds(e, 1), :] = scales[:, pl.ds(pl.multiple_of(me * width, width), width)]

        def body(r, carry):
            at = pl.ds(pl.multiple_of(r * STEP, STEP), STEP)
            for c in range(n):
                lanes = slice(c * width, (c + 1) * width)
                sendbuf[m, e, c, at, :] = (src[at, lanes] / scale[:, lanes]).astype(jnp.bfloat16)
            return carry

        lax.fori_loop(0, rows // STEP, body, 0, unroll=2)

    def place(ref, e, s):
        return ref.at[e, pl.ds(pl.multiple_of(s * rows, rows), rows), :]

    def keep(m, e):
        pltpu.make_async_copy(sendbuf.at[m, e, me], place(o[m], e, me), own_sem.at[m]).start()

    def send(m, e, p):
        pltpu.make_async_remote_copy(
            src_ref=sendbuf.at[m, e, p], dst_ref=place(o[m], e, me),
            send_sem=send_sem.at[m, p], recv_sem=recv_sem.at[m, me],
            device_id={"zero": p}, device_id_type=MESH,
        ).start()

    def send_at(m, e, t):
        @pl.when(me + t < n)
        def _():
            send(m, e, me + t)

        @pl.when(me - t >= 0)
        def _():
            send(m, e, me - t)

    for m in range(2):
        pltpu.make_async_copy(w[m].at[0], first.at[m], first_sem.at[m]).wait()
        stats(first.at[m], m, 0)
        if m == 0:
            pl.semaphore_wait(barrier, n - 1 + banks - 1)
        others("zero", me, n, lambda p: swap(m, p).start())

    def arrived(g):
        others("zero", me, n, lambda p: swapped(g, p).wait_recv())

    arrived(0)
    narrow(first.at[0], 0, 0)
    for t in range(1, n):
        send_at(0, 0, t)
    keep(0, 0)

    depth = rw_ref.shape[1]
    mine = pl.ds(pl.multiple_of(me * depth, depth), depth)
    rt_ref[bank, :, mine] = (rw_ref[...] * rg_ref[...]).astype(jnp.bfloat16)

    def row_copy(s, p):
        at = pl.ds(pl.multiple_of(s * depth, depth), depth)
        return pltpu.make_async_remote_copy(
            src_ref=rt_ref.at[bank, :, at], dst_ref=rt_ref.at[bank, :, at],
            send_sem=rz_send.at[p], recv_sem=rz_recv.at[s],
            device_id={"zero": p}, device_id_type=MESH,
        )

    def sizes(e, carry):
        slot = e % SLOTS
        for m in range(2):
            load(m, e, slot).wait()
            stats(stage.at[m, slot], m, e)

            @pl.when(e + SLOTS < experts)
            def _():
                load(m, e + SLOTS, slot).start()
        return carry

    lax.fori_loop(1, experts, sizes, 0)
    others("zero", me, n, lambda p: swap(2, p).start())
    for e in range(1, min(1 + SLOTS, experts)):
        for m in range(2):
            load(m, e, e % SLOTS).start()

    arrived(1)
    narrow(first.at[1], 1, 0)
    for t in range(1, n):
        send_at(1, 0, t)
    keep(1, 0)
    others("zero", me, n, lambda p: row_copy(me, p).start())

    arrived(2)

    def narrowed(e, carry):
        slot = e % SLOTS
        for m in range(2):
            load(m, e, slot).wait()
            narrow(stage.at[m, slot], m, e)

            @pl.when(e + SLOTS < experts)
            def _():
                load(m, e + SLOTS, slot).start()

            send_at(m, e, 1)
            keep(m, e)
        return carry

    lax.fori_loop(1, experts, narrowed, 0)

    def far(e, carry):
        for m in range(2):
            for t in range(2, n):
                send_at(m, e, t)
        return carry

    lax.fori_loop(1, experts, far, 0)

    others("zero", me, n, lambda p: row_copy(p, p).wait_recv())

    def column_copy(s, p):
        return pltpu.make_async_remote_copy(
            src_ref=rt_ref.at[s], dst_ref=rt_ref.at[s],
            send_sem=rb_send.at[p], recv_sem=rb_recv.at[s],
            device_id={"bank": p}, device_id_type=MESH,
        )

    others("bank", bank, banks, lambda p: column_copy(bank, p).start())
    others("bank", bank, banks, lambda p: column_copy(p, p).wait_recv())
    others("bank", bank, banks, lambda p: column_copy(bank, p).wait_send())
    others("zero", me, n, lambda p: row_copy(me, p).wait_send())
    for g in range(3):
        others("zero", me, n, lambda p: swap(g, p).wait_send())

    for m in range(2):
        def whole(s, p):
            return pltpu.make_async_remote_copy(
                src_ref=sendbuf.at[m, :, p],
                dst_ref=o[m].at[:, pl.ds(pl.multiple_of(s * rows, rows), rows), :],
                send_sem=send_sem.at[m, p], recv_sem=recv_sem.at[m, s],
                device_id={"zero": p}, device_id_type=MESH,
            )

        pltpu.make_async_copy(
            sendbuf.at[m, :, me], o[m].at[:, pl.ds(pl.multiple_of(me * rows, rows), rows), :], own_sem.at[m]
        ).wait()
        others("zero", me, n, lambda p: whole(me, p).wait_send())
        others("zero", me, n, lambda p: whole(p, p).wait_recv())


def local(n, banks, w_gate, w_up, router_weight, router_gain):
    experts, rows, cols = w_gate.shape
    width = cols // n
    depth, heads = router_weight.shape
    fits = width % 128 == 0 and rows % 16 == 0 and depth % 128 == 0 and heads % 16 == 0 and experts > 1
    if not fits:
        return plain(n, w_gate, w_up, router_weight, router_gain)
    anywhere = pl.BlockSpec(memory_space=pl.ANY)
    vmem = pl.BlockSpec(memory_space=pltpu.VMEM)
    dma = pltpu.SemaphoreType.DMA
    serve = jax.ShapeDtypeStruct((experts, rows * n, width), jnp.bfloat16)
    scale = jax.ShapeDtypeStruct((experts, width), jnp.float32)
    og, ou, sg, su, rt = pl.pallas_call(
        functools.partial(kernel, n, banks),
        out_shape=(serve, serve, scale, scale, jax.ShapeDtypeStruct((banks, heads, depth * n), jnp.bfloat16)),
        in_specs=[anywhere, anywhere, vmem, vmem],
        out_specs=(anywhere, anywhere, vmem, vmem, vmem),
        scratch_shapes=[
            pltpu.VMEM((2, SLOTS, rows, cols), jnp.float32),
            pltpu.VMEM((2, rows, cols), jnp.float32),
            pltpu.VMEM((2, experts, n, rows, width), jnp.bfloat16),
            pltpu.VMEM((n, experts, 2, 1, cols), jnp.float32),
            pltpu.VMEM((1, cols), jnp.float32),
            dma((2, SLOTS)), dma((2,)), dma((2,)), dma((2, n)), dma((2, n)),
            dma((3, n)), dma((3, n)), dma((n,)), dma((n,)), dma((banks,)), dma((banks,)),
        ],
        compiler_params=pltpu.CompilerParams(
            collective_id=0, has_side_effects=True, vmem_limit_bytes=58 * 1024 * 1024
        ),
    )(w_gate, w_up, router_weight.T, router_gain[None, :])
    return og, ou, sg, su, rt.reshape(banks * heads, depth * n).T


def solution(mesh):
    n, banks = mesh.shape["zero"], mesh.shape["bank"]
    return jax.shard_map(
        functools.partial(local, n, banks),
        mesh=mesh,
        in_specs=(
            P(("trial", "bank"), "zero", None),
            P(("trial", "bank"), "zero", None),
            P(("trial", "zero"), "bank"),
            P(("trial", "zero")),
        ),
        out_specs=(
            P(("trial", "bank"), None, "zero"),
            P(("trial", "bank"), None, "zero"),
            P(("trial", "bank"), "zero"),
            P(("trial", "bank"), "zero"),
            P("trial", None),
        ),
        check_vma=False,
    )
```

```python
import functools

import jax
import jax.numpy as jnp
from jax import lax
from jax.experimental import pallas as pl
from jax.experimental.pallas import tpu as pltpu
from jax.sharding import PartitionSpec as P

MESH = pl.DeviceIdType.MESH
SLOTS = 3
STEP = 16


def plain(n, w_gate, w_up, router_weight, router_gain):
    d_model = w_gate.shape[1] * n

    def rescaled(w):
        scale = lax.psum(jnp.sum(jnp.abs(w), axis=1), "zero") / d_model
        narrow = (w / jnp.expand_dims(scale, 1)).astype(jnp.bfloat16)
        serve = lax.all_to_all(narrow, "zero", split_axis=2, concat_axis=1, tiled=True)
        width = serve.shape[2]
        return serve, lax.dynamic_slice_in_dim(scale, lax.axis_index("zero") * width, width, axis=1)

    serve_gate, scale_gate = rescaled(w_gate)
    serve_up, scale_up = rescaled(w_up)
    part = (router_weight * router_gain[:, None]).astype(jnp.bfloat16)
    row = lax.all_gather(part, "zero", axis=0, tiled=True)
    router = lax.all_gather(row, "bank", axis=1, tiled=True)
    return serve_gate, serve_up, scale_gate, scale_up, router


def kernel(
    n, banks, wg_ref, wu_ref, rw_ref, rg_ref, *refs
):
    og_ref, ou_ref, sg_ref, su_ref, rt_ref = refs[:5]
    tails = refs[5 : 5 + n]
    stage, first, sendbuf, parts, scales = refs[5 + n : 10 + n]
    (
    tail_sem, in_sem, first_sem, own_sem, send_sem, recv_sem, x_send, x_recv, rz_send, rz_recv, rb_send, rb_recv,
    ) = refs[10 + n :]
    me = lax.axis_index("zero")
    bank = lax.axis_index("bank")
    w, o, so = (wg_ref, wu_ref), (og_ref, ou_ref), (sg_ref, su_ref)
    experts, rows, cols = wg_ref.shape
    width = cols // n
    d_model = rows * n
    last = experts - 1

    for m in range(2):
        pltpu.make_async_copy(w[m].at[0], first.at[m], first_sem.at[m]).start()

    def load(m, e, slot):
        return pltpu.make_async_copy(w[m].at[e], stage.at[m, slot], in_sem.at[m, slot])

    for e in range(1, min(1 + SLOTS, experts)):
        for m in range(2):
            load(m, e, e % SLOTS).start()

    def others(axis, here, count, act):
        for p in range(count):
            @pl.when(here != p)
            def _():
                act(p)

    barrier = pltpu.get_barrier_semaphore()

    def greet(axis):
        return lambda p: pl.semaphore_signal(barrier, inc=1, device_id={axis: p}, device_id_type=MESH)

    others("zero", me, n, greet("zero"))
    others("bank", bank, banks, greet("bank"))

    def stats(src, m, e):
        def body(r, acc):
            return acc + jnp.abs(src[pl.ds(pl.multiple_of(r * 8, 8), 8), :])

        acc = lax.fori_loop(0, rows // 8, body, jnp.zeros((8, cols), jnp.float32), unroll=8)
        parts[me, e, m] = jnp.sum(acc, axis=0, keepdims=True)

    def chunk(ref, s, g):
        if g < 2:
            return ref.at[s, 0, g]
        return ref.at[s, pl.ds(1, experts - 1)]

    def swap(g, p):
        return pltpu.make_async_remote_copy(
            src_ref=chunk(parts, me, g), dst_ref=chunk(parts, me, g),
            send_sem=x_send.at[g, p], recv_sem=x_recv.at[g, me],
            device_id={"zero": p}, device_id_type=MESH,
        )

    def swapped(g, p):
        return pltpu.make_async_remote_copy(
            src_ref=chunk(parts, p, g), dst_ref=chunk(parts, p, g),
            send_sem=x_send.at[g, p], recv_sem=x_recv.at[g, p],
            device_id={"zero": p}, device_id_type=MESH,
        )

    def narrow(src, m, e):
        total = parts[0, e, m]
        for s in range(1, n):
            total = total + parts[s, e, m]
        scale = total / d_model
        scales[...] = scale
        so[m][pl.ds(e, 1), :] = scales[:, pl.ds(pl.multiple_of(me * width, width), width)]

        def body(r, carry):
            at = pl.ds(pl.multiple_of(r * STEP, STEP), STEP)
            for c in range(n):
                lanes = slice(c * width, (c + 1) * width)
                sendbuf[m, e, c, at, :] = (src[at, lanes] / scale[:, lanes]).astype(jnp.bfloat16)
            return carry

        lax.fori_loop(0, rows // STEP, body, 0, unroll=2)

    def place(ref, e, s):
        return ref.at[e, pl.ds(pl.multiple_of(s * rows, rows), rows), :]

    def keep(m, e):
        pltpu.make_async_copy(sendbuf.at[m, e, me], place(o[m], e, me), own_sem.at[m]).start()

    def send(m, e, p):
        pltpu.make_async_remote_copy(
            src_ref=sendbuf.at[m, e, p], dst_ref=place(o[m], e, me),
            send_sem=send_sem.at[m, p], recv_sem=recv_sem.at[m, me],
            device_id={"zero": p}, device_id_type=MESH,
        ).start()

    def send_at(m, e, t):
        @pl.when(me + t < n)
        def _():
            send(m, e, me + t)

        @pl.when(me - t >= 0)
        def _():
            send(m, e, me - t)

    for m in range(2):
        pltpu.make_async_copy(w[m].at[0], first.at[m], first_sem.at[m]).wait()
        stats(first.at[m], m, 0)
        if m == 0:
            pl.semaphore_wait(barrier, n - 1 + banks - 1)
        others("zero", me, n, lambda p: swap(m, p).start())

    def arrived(g):
        others("zero", me, n, lambda p: swapped(g, p).wait_recv())

    arrived(0)
    narrow(first.at[0], 0, 0)
    for t in range(1, n):
        send_at(0, 0, t)
    keep(0, 0)

    depth = rw_ref.shape[1]
    mine = pl.ds(pl.multiple_of(me * depth, depth), depth)
    rt_ref[bank, :, mine] = (rw_ref[...] * rg_ref[...]).astype(jnp.bfloat16)

    def row_copy(s, p):
        at = pl.ds(pl.multiple_of(s * depth, depth), depth)
        return pltpu.make_async_remote_copy(
            src_ref=rt_ref.at[bank, :, at], dst_ref=rt_ref.at[bank, :, at],
            send_sem=rz_send.at[p], recv_sem=rz_recv.at[s],
            device_id={"zero": p}, device_id_type=MESH,
        )

    def sizes(e, carry):
        slot = e % SLOTS
        for m in range(2):
            load(m, e, slot).wait()
            stats(stage.at[m, slot], m, e)

            @pl.when(e + SLOTS < experts)
            def _():
                load(m, e + SLOTS, slot).start()
        return carry

    lax.fori_loop(1, experts, sizes, 0)
    others("zero", me, n, lambda p: swap(2, p).start())
    for e in range(1, min(1 + SLOTS, experts)):
        for m in range(2):
            load(m, e, e % SLOTS).start()

    arrived(1)
    narrow(first.at[1], 1, 0)
    for t in range(1, n):
        send_at(1, 0, t)
    keep(1, 0)
    others("zero", me, n, lambda p: row_copy(me, p).start())

    arrived(2)

    def put(m, d):
        return pltpu.make_async_copy(
            sendbuf.at[m, last, lax.rem(me + d, n)], tails[d].at[m], tail_sem.at[d, m]
        )

    def narrowed(e, carry):
        slot = e % SLOTS
        for m in range(2):
            load(m, e, slot).wait()
            narrow(stage.at[m, slot], m, e)

            @pl.when(e + SLOTS < experts)
            def _():
                load(m, e + SLOTS, slot).start()

            @pl.when(e < last)
            def _():
                send_at(m, e, 1)
                keep(m, e)
        return carry

    lax.fori_loop(1, experts, narrowed, 0)
    for m in range(2):
        for d in range(n):
            put(m, d).start()

    def far(e, carry):
        for m in range(2):
            for t in range(2, n):
                send_at(m, e, t)
        return carry

    lax.fori_loop(1, last, far, 0)
    for m in range(2):
        for d in range(n):
            put(m, d).wait()

    others("zero", me, n, lambda p: row_copy(p, p).wait_recv())

    def column_copy(s, p):
        return pltpu.make_async_remote_copy(
            src_ref=rt_ref.at[s], dst_ref=rt_ref.at[s],
            send_sem=rb_send.at[p], recv_sem=rb_recv.at[s],
            device_id={"bank": p}, device_id_type=MESH,
        )

    others("bank", bank, banks, lambda p: column_copy(bank, p).start())
    others("bank", bank, banks, lambda p: column_copy(p, p).wait_recv())
    others("bank", bank, banks, lambda p: column_copy(bank, p).wait_send())
    others("zero", me, n, lambda p: row_copy(me, p).wait_send())
    for g in range(3):
        others("zero", me, n, lambda p: swap(g, p).wait_send())

    for m in range(2):
        def whole(s, p):
            return pltpu.make_async_remote_copy(
                src_ref=sendbuf.at[m, pl.ds(0, last), p],
                dst_ref=o[m].at[:, pl.ds(pl.multiple_of(s * rows, rows), rows), :],
                send_sem=send_sem.at[m, p], recv_sem=recv_sem.at[m, s],
                device_id={"zero": p}, device_id_type=MESH,
            )

        pltpu.make_async_copy(
            sendbuf.at[m, pl.ds(0, last), me], o[m].at[:, pl.ds(pl.multiple_of(me * rows, rows), rows), :], own_sem.at[m]
        ).wait()
        others("zero", me, n, lambda p: whole(me, p).wait_send())
        others("zero", me, n, lambda p: whole(p, p).wait_recv())


def copy_kernel(a_ref, b_ref, c_ref, d_ref):
    c_ref[...] = a_ref[...]
    d_ref[...] = b_ref[...]


def spread(experts, og, ou):
    main, height, width = og.shape
    block = pl.BlockSpec((1, height, width), lambda e: (e, 0, 0))
    out = jax.ShapeDtypeStruct((experts, height, width), og.dtype)
    return pl.pallas_call(
        copy_kernel,
        grid=(main,),
        in_specs=[block, block],
        out_specs=(block, block),
        out_shape=(out, out),
        cost_estimate=pl.CostEstimate(flops=0, bytes_accessed=8 * og.size, transcendentals=0),
        name="spread",
    )(og, ou)


def join_kernel(n, a_ref, b_ref, *refs):
    blocks, outs, sem = refs[:n], refs[n : n + 2], refs[n + 2]
    me = lax.axis_index("zero")
    last = outs[0].shape[0] - 1
    rows = blocks[0].shape[1]
    copies = []
    for d in range(n):
        at = pl.ds(pl.multiple_of(lax.rem(me - d + n, n) * rows, rows), rows)
        for m in range(2):
            copies.append(pltpu.make_async_copy(blocks[d].at[m], outs[m].at[last, at, :], sem.at[d, m]))
    for copy in copies:
        copy.start()
    for copy in copies:
        copy.wait()


def join(n, og, ou, blocks):
    anywhere = pl.BlockSpec(memory_space=pl.ANY)
    vmem = pl.BlockSpec(memory_space=pltpu.VMEM)
    return pl.pallas_call(
        functools.partial(join_kernel, n),
        out_shape=(jax.ShapeDtypeStruct(og.shape, og.dtype), jax.ShapeDtypeStruct(ou.shape, ou.dtype)),
        in_specs=[anywhere, anywhere] + [vmem] * n,
        out_specs=(anywhere, anywhere),
        scratch_shapes=[pltpu.SemaphoreType.DMA((n, 2))],
        input_output_aliases={0: 0, 1: 1},
        name="join",
    )(og, ou, *blocks)


def local(n, banks, w_gate, w_up, router_weight, router_gain):
    experts, rows, cols = w_gate.shape
    width = cols // n
    depth, heads = router_weight.shape
    fits = width % 128 == 0 and rows % 16 == 0 and depth % 128 == 0 and heads % 16 == 0 and experts > 2
    if not fits:
        return plain(n, w_gate, w_up, router_weight, router_gain)
    anywhere = pl.BlockSpec(memory_space=pl.ANY)
    vmem = pl.BlockSpec(memory_space=pltpu.VMEM)
    dma = pltpu.SemaphoreType.DMA
    serve = jax.ShapeDtypeStruct((experts - 1, rows * n, width), jnp.bfloat16)
    tail = jax.ShapeDtypeStruct((2, rows, width), jnp.bfloat16)
    scale = jax.ShapeDtypeStruct((experts, width), jnp.float32)
    og, ou, sg, su, rt, *tails = pl.pallas_call(
        functools.partial(kernel, n, banks),
        out_shape=(serve, serve, scale, scale, jax.ShapeDtypeStruct((banks, heads, depth * n), jnp.bfloat16), *[tail] * n),
        in_specs=[anywhere, anywhere, vmem, vmem],
        out_specs=(anywhere, anywhere, vmem, vmem, vmem, *[anywhere] * n),
        scratch_shapes=[
            pltpu.VMEM((2, SLOTS, rows, cols), jnp.float32),
            pltpu.VMEM((2, rows, cols), jnp.float32),
            pltpu.VMEM((2, experts, n, rows, width), jnp.bfloat16),
            pltpu.VMEM((n, experts, 2, 1, cols), jnp.float32),
            pltpu.VMEM((1, cols), jnp.float32),
            dma((n, 2)), dma((2, SLOTS)), dma((2,)), dma((2,)), dma((2, n)), dma((2, n)),
            dma((3, n)), dma((3, n)), dma((n,)), dma((n,)), dma((banks,)), dma((banks,)),
        ],
        compiler_params=pltpu.CompilerParams(
            collective_id=0, has_side_effects=True, vmem_limit_bytes=58 * 1024 * 1024
        ),
    )(w_gate, w_up, router_weight.T, router_gain[None, :])
    arrived = [tails[0]] + [
        lax.ppermute(tails[d], "zero", [(i, (i + d) % n) for i in range(n)]) for d in range(1, n)
    ]
    og, ou = spread(experts, og, ou)
    og, ou = join(n, og, ou, arrived)
    return og, ou, sg, su, rt.reshape(banks * heads, depth * n).T


def solution(mesh):
    n, banks = mesh.shape["zero"], mesh.shape["bank"]
    return jax.shard_map(
        functools.partial(local, n, banks),
        mesh=mesh,
        in_specs=(
            P(("trial", "bank"), "zero", None),
            P(("trial", "bank"), "zero", None),
            P(("trial", "zero"), "bank"),
            P(("trial", "zero")),
        ),
        out_specs=(
            P(("trial", "bank"), None, "zero"),
            P(("trial", "bank"), None, "zero"),
            P(("trial", "bank"), "zero"),
            P(("trial", "bank"), "zero"),
            P("trial", None),
        ),
        check_vma=False,
    )
```
